32 devices in a mesh: level: 4 (over x, core), body: 8 (over z, y).
Axes of the slice: x: 2, y: 2, z: 4, core: 2. Of those that a mesh axis runs over, the one named last changes fastest.
Arguments:
- state: float32 [4, 6, 8192], P('level', None, 'body'), may hold values from -14 to 14
- history: float32 [4, 3, 6, 8192], P('level', None, None, 'body'), may hold values from -6 to 6
- masses: float32 [8192], P('body'), may hold values from 0.25 to 4
Outputs:
- final_state: float32 [4, 6, 8192], P('level', None, 'body')
The draws below stay inside these ranges and needn't reach their ends.
All inputs are finite; a program needn't handle non-finite values.
Results may differ from the reference program's by a relative error of at most 0.0001.
Values sent between devices are 32-bit elements; how exact they have to be, the bound alone decides.
A program may use at most 64 MiB of HBM per device.

```python
import math
import jax
import jax.numpy as jnp
from jax import lax

LEVELS = 4
STEPS = 4
BODIES = 8192


def draw_state(key, part):
    key = jax.random.fold_in(key, 17)
    keys = jax.random.split(key, 6)
    positions = jnp.clip(jax.random.normal(keys[4], (LEVELS, 3, BODIES), jnp.float32), -6.0, 6.0)
    velocities = jnp.clip(jax.random.normal(keys[5], (LEVELS, 3, BODIES), jnp.float32), -6.0, 6.0)
    return jnp.concatenate([positions, velocities], axis=1).astype(jnp.float32)


def levels(key, shape, pieces, low, high):
    gain = 1.0
    for axis_at, parts in pieces:
        draws = jax.random.uniform(jax.random.fold_in(jax.random.fold_in(key, 6), axis_at), (parts,), jnp.float32, low / len(pieces), high / len(pieces))
        gain = gain * jnp.repeat(jnp.exp(draws), shape[axis_at] // parts).reshape((-1,) + (1,) * (len(shape) - 1 - axis_at))
    return gain


def gaussian(rng, extent, scale, bound, cuts=(), held_as=jnp.bfloat16):
    entries = jax.random.normal(rng, extent, jnp.float32) * scale
    if len(cuts) > 0:
        entries = levels(rng, extent, cuts, -0.22, 0.18) * entries
    return jnp.clip(entries, min=-bound, max=bound).astype(held_as)


def setup_inputs(seed: int = 0) -> dict:
    arg_keys = jax.random.split(jax.random.key(seed), 4)
    return {
        "state": draw_state(jax.random.fold_in(arg_keys[3], 71), 0),
        "history": gaussian(arg_keys[1], (LEVELS, 3, 6, BODIES), 1.0, 6.0, ((0, 4), (3, 8)), jnp.float32),
        "masses": jnp.clip(jnp.exp(math.log(4.0) - 2.7725887 * jax.random.uniform(arg_keys[2], (BODIES,), jnp.float32) ** levels(arg_keys[2], (BODIES,), ((0, 8),), -0.2, 0.2)), 0.25, 4.0),
    }


SOFTEN = 0.05
DELTA = 0.05
COUPLING = 512.0

def accelerate(positions, masses):
    block_size = min(BODIES, 1024)

    def one_block(targets):
        offsets = positions[:, None, :] - targets[:, :, None]
        distance = lax.optimization_barrier(jnp.sum(offsets * offsets, axis=0)) + SOFTEN
        weight = masses[None, :] / (distance * jnp.sqrt(distance))
        return lax.optimization_barrier(jnp.sum(offsets * weight[None], axis=2))
    tile_list = positions.reshape(3, BODIES // block_size, block_size).transpose(1, 0, 2)
    pull_tiles = lax.map(one_block, tile_list)
    return pull_tiles.transpose(1, 0, 2).reshape(3, BODIES) * (COUPLING / BODIES)

def reference(state, history, masses):
    current = state
    stored = history
    for repeat_index in range(STEPS):
        forces = jnp.stack([jnp.concatenate([current[level_index, 3:6], accelerate(current[level_index, 0:3], masses)], axis=0) for level_index in range(LEVELS)])
        updated = [current[0] + DELTA * forces[0]]
        retained = [stored[0]]
        for level_index in range(1, LEVELS):
            history_rows = stored[level_index]
            quadrature = history_rows[0] / 24.0 - 5.0 * history_rows[1] / 24.0 + 19.0 * history_rows[2] / 24.0 + 9.0 * forces[level_index - 1] / 24.0
            updated.append(current[level_index] + DELTA * (forces[level_index] - history_rows[2]) + DELTA * quadrature)
            retained.append(jnp.stack([history_rows[1], history_rows[2], forces[level_index - 1]]))
        current = jnp.stack(updated)
        stored = jnp.stack(retained)
    return current
```

```python
import functools

import jax
import jax.numpy as jnp
from jax import lax
from jax.experimental import pallas as pl
from jax.experimental.pallas import tpu as pltpu
from jax.sharding import PartitionSpec as P

STEPS = 4
SOFTEN = 0.05
DELTA = 0.05
COUPLING = 512.0
BF16 = jnp.bfloat16
F32 = jnp.float32
TILE = 256
SIDES = 2
LEAD = 3


def split_in_three(x):
    high = x.astype(BF16).astype(F32)
    rest = x - high
    middle = rest.astype(BF16).astype(F32)
    return high, middle, rest - middle


def corrected(current, force, past, lower, level):
    oldest, middle, newest = past
    quadrature = (
        oldest / 24.0 - 5.0 * middle / 24.0 + 19.0 * newest / 24.0 + 9.0 * lower / 24.0
    )
    return jnp.where(
        level == 0,
        current + DELTA * force,
        current + DELTA * (force - newest) + DELTA * quadrature,
    )


def kernel(ring, levels, *refs):
    count = refs[0].shape[1]
    accumulators = []
    for side in range(SIDES):
        accumulators += [pltpu.ACC(side)((TILE, TILE), F32)] * 2
        accumulators += [pltpu.ACC(side)((16, TILE), F32)] * (count // TILE)

    def scoped(*held):
        each = len(held) // SIDES
        sides = (held[:each], held[each:])
        window(ring, levels, [s[:2] for s in sides], [s[2:] for s in sides], *refs)

    pl.run_scoped(scoped, *accumulators)


def window(
    ring, levels, far, near, state, history, masses, out,
    blocks, left_even, left_odd, right_even, right_odd, target_pieces, vel, acc, hist_v, hist_a, low_hist,
    pos, sums, target_rows, source_rows,
    pos_send, pos_recv, acc_send, acc_recv, low_send, low_recv,
):
    count = state.shape[1]
    tiles = count // TILE
    level = lax.axis_index("level")
    me = lax.axis_index("body")
    total_turns = STEPS * ring
    left = (left_even, left_odd)
    right = (right_even, right_odd)

    def above(distance):
        return lax.rem(level + distance, levels)

    def peer(k):
        half = (k + 1) // 2
        return lax.rem(me + ring + half * (2 * lax.rem(k, 2) - 1), ring)

    def pos_copy(step, k):
        return pltpu.make_async_remote_copy(
            src_ref=blocks.at[step, me, 0:4],
            dst_ref=blocks.at[step, me, 0:4],
            send_sem=pos_send.at[step, k],
            recv_sem=pos_recv.at[step, me],
            device_id=(level, peer(k)),
            device_id_type=pl.DeviceIdType.MESH,
        )

    def pos_arrival(step, owner):
        return pltpu.make_async_remote_copy(
            src_ref=blocks.at[step, owner, 0:4],
            dst_ref=blocks.at[step, owner, 0:4],
            send_sem=pos_send.at[step, 0],
            recv_sem=pos_recv.at[step, owner],
            device_id=(level, owner),
            device_id_type=pl.DeviceIdType.MESH,
        )

    def acc_copy(step, distance):
        target = (hist_a, low_hist)[distance - 1]
        return pltpu.make_async_remote_copy(
            src_ref=acc.at[step],
            dst_ref=target.at[step + 3],
            send_sem=acc_send.at[distance - 1, step],
            recv_sem=acc_recv.at[distance - 1, step],
            device_id=(above(distance), me),
            device_id_type=pl.DeviceIdType.MESH,
        )

    def low_copy():
        return pltpu.make_async_remote_copy(
            src_ref=vel.at[0],
            dst_ref=hist_v.at[3],
            send_sem=low_send.at[0],
            recv_sem=low_recv.at[0],
            device_id=(above(1), me),
            device_id_type=pl.DeviceIdType.MESH,
        )

    def low_hist_copy():
        return pltpu.make_async_remote_copy(
            src_ref=hist_a.at[0:3],
            dst_ref=low_hist.at[0:3],
            send_sem=low_send.at[1],
            recv_sem=low_recv.at[1],
            device_id=(above(1), me),
            device_id_type=pl.DeviceIdType.MESH,
        )

    def broadcast(step):
        def one(k, carry):
            pos_copy(step, k).start()
            return carry
        lax.fori_loop(1, ring, one, 0)

    barrier = pltpu.get_barrier_semaphore()

    def greet(k, carry):
        pl.semaphore_signal(
            barrier, inc=1, device_id=(level, peer(k)), device_id_type=pl.DeviceIdType.MESH
        )
        return carry

    lax.fori_loop(1, ring, greet, 0)

    def greet_level(distance, carry):
        pl.semaphore_signal(
            barrier, inc=1, device_id=(above(distance), me), device_id_type=pl.DeviceIdType.MESH
        )
        return carry

    lax.fori_loop(1, levels, greet_level, 0)
    pos[...] = state[0:3]
    blocks[0, me, 0:3] = state[0:3]
    for step in range(STEPS):
        blocks[step, me, 3:4] = masses[...]
    vel[0] = state[3:6]
    for k in range(3):
        hist_v[k] = history[k, 0:3]
        hist_a[k] = history[k, 3:6]
    pl.semaphore_wait(barrier, ring - 1 + levels - 1)
    broadcast(0)
    low_copy().start()
    low_hist_copy().start()

    def next_position(step):
        past = (hist_v[step], hist_v[step + 1], hist_v[step + 2])
        return corrected(pos[...], vel[step], past, hist_v[step + 3], level)

    def next_velocity(step):
        acc_copy(step, 1).wait_recv()
        past = (hist_a[step], hist_a[step + 1], hist_a[step + 2])
        vel[step + 1] = corrected(vel[step], acc[step], past, hist_a[step + 3], level)

    def next_low_velocity(step):
        acc_copy(step, 2).wait_recv()
        past = (low_hist[step], low_hist[step + 1], low_hist[step + 2])
        hist_v[step + 4] = corrected(
            hist_v[step + 3], hist_a[step + 3], past, low_hist[step + 3], level - 1
        )

    def publish(step):
        moved = next_position(step - 1)
        pos[...] = moved
        blocks[step, me, 0:3] = moved
        prepare_targets(step)

    def augmented(step, owner):
        p = blocks[step, owner, 0:3]
        return p, jnp.sum(p * p, axis=0, keepdims=True), blocks[step, owner, 3:4]

    def prepare_targets(step):
        p, square, _ = augmented(step, me)
        target_rows[0:3] = -2.0 * p
        target_rows[4:5] = square + SOFTEN
        high, middle, low = split_in_three(target_rows[...])
        target_pieces[lax.rem(step, 2)] = jnp.concatenate(
            [high, middle, high, low, high, middle], axis=0
        ).astype(BF16)

    def prepare_sources(slot, step, owner):
        p, square, mass = augmented(step, owner)
        source_rows[0:3] = p
        source_rows[3:4] = square
        source = source_rows[...]
        high, middle, low = split_in_three(source)
        rows = [high, high, middle, high, low, middle, jnp.zeros((80, count), F32)]
        left[slot][...] = jnp.concatenate(rows, axis=0).astype(BF16).T
        moments = source * mass
        coarse = moments.astype(BF16).astype(F32)
        right[slot][...] = jnp.concatenate([coarse, moments - coarse], axis=0).astype(BF16)

    rounds = [(j, i) for j in range(tiles) for i in range(tiles)]
    registers = [0] * SIDES

    def stage(value, side):
        register = registers[side]
        registers[side] = 1 - register
        pltpu.matmul_push_rhs(value, staging_register=register, mxu_index=side)
        return register

    def buffer(index):
        return far[index % SIDES][(index // SIDES) % 2]

    def distances(index, slot, step):
        j, i = rounds[index]
        at = i * TILE
        pieces = target_pieces[lax.rem(step, 2), :, at:at + TILE]
        pieces = jnp.concatenate([pieces, jnp.zeros((TILE - 48, TILE), BF16)], axis=0)
        lhs = left[slot][j * TILE:(j + 1) * TILE]
        lhs = jnp.concatenate([lhs, jnp.zeros((TILE, 128), BF16)], axis=1)
        register = stage(pieces, index % SIDES)
        pltpu.matmul_acc_lhs(buffer(index), lhs, load_staged_rhs=register)

    def pulls(index, slot):
        j, i = rounds[index]
        part = right[slot][:, j * TILE:(j + 1) * TILE]
        inverse = lax.rsqrt(pltpu.matmul_pop(buffer(index)))
        weight = inverse * inverse * inverse
        weight_high = weight.astype(BF16)
        weight_low = weight - weight_high.astype(F32)
        for side, piece in enumerate((weight_high, weight_low)):
            register = stage(piece, side)
            pltpu.matmul_acc_lhs(near[side][i], part, load_staged_rhs=register)

    def add_block(slot, step, next_step):
        for index in range(len(rounds)):
            ahead = index + LEAD
            if ahead < len(rounds):
                distances(ahead, slot, step)
            else:
                distances(ahead - len(rounds), 1 - slot, next_step)
            pulls(index, slot)

    for side in range(SIDES):
        for used in far[side] + near[side]:
            pltpu.matmul_pop(used)

    def finish(step):
        for i in range(tiles):
            high = pltpu.matmul_pop(near[0][i])
            sums[:, i * TILE:(i + 1) * TILE] = high + pltpu.matmul_pop(near[1][i])
        total = sums[0:8] + sums[8:16]
        own = blocks[step, me, 0:3]
        acc[step] = (total[0:3] - own * total[4:5]) * (COUPLING / (count * ring))

    target_rows[...] = jnp.zeros((8, count), F32)
    target_rows[3:4] = jnp.ones((1, count), F32)
    source_rows[...] = jnp.zeros((8, count), F32)
    source_rows[4:5] = jnp.ones((1, count), F32)
    prepare_targets(0)
    prepare_sources(0, 0, me)
    for index in range(LEAD):
        distances(index, 0, 0)

    def one_turn(turn, slot):
        step = turn // ring
        k = lax.rem(turn, ring)
        after = lax.rem(turn + 1, total_turns)
        next_step = after // ring
        next_k = lax.rem(after, ring)

        if slot == 1:
            @pl.when(k == 1)
            def _():
                @pl.when(step > 0)
                def _():
                    acc_copy(step - 1, 1).start()
                    acc_copy(step - 1, 2).start()

                @pl.when(step == 0)
                def _():
                    low_copy().wait_recv()
                    publish(1)

            @pl.when((k == 5) & (step > 0) & (step < STEPS - 1))
            def _():
                broadcast(step + 1)
        else:
            @pl.when((k == 2) & (step == 0))
            def _():
                low_hist_copy().wait_recv()
                broadcast(1)

            @pl.when((k == 4) & (step > 0))
            def _():
                next_velocity(step - 1)
                next_low_velocity(step - 1)

                @pl.when(step < STEPS - 1)
                def _():
                    publish(step + 1)

        @pl.when(next_k > 0)
        def _():
            pos_arrival(next_step, peer(next_k)).wait_recv()

        prepare_sources(1 - slot, next_step, peer(next_k))
        add_block(slot, step, next_step)

        if slot == 1:
            @pl.when(k == ring - 1)
            def _():
                finish(step)

    def two_turns(pair, carry):
        one_turn(2 * pair, 0)
        one_turn(2 * pair + 1, 1)
        return carry

    lax.fori_loop(0, total_turns // 2, two_turns, 0)
    for index in range(LEAD):
        pltpu.matmul_pop(buffer(index))
    acc_copy(STEPS - 1, 1).start()
    out[0:3] = next_position(STEPS - 1)
    next_velocity(STEPS - 1)
    out[3:6] = vel[STEPS]

    def drain(step, carry):
        def one(k, inner):
            pos_copy(step, k).wait_send()
            return inner
        lax.fori_loop(1, ring, one, 0)
        acc_copy(step, 1).wait_send()

        @pl.when(step < STEPS - 1)
        def _():
            acc_copy(step, 2).wait_send()

        return carry

    lax.fori_loop(0, STEPS, drain, 0)
    low_copy().wait_send()
    low_hist_copy().wait_send()


def solution(mesh):
    ring = mesh.shape["body"]
    levels = mesh.shape["level"]

    def on_device(state, history, masses):
        count = state.shape[2]
        dma = pltpu.SemaphoreType.DMA
        rows = pltpu.VMEM
        result = pl.pallas_call(
            functools.partial(kernel, ring, levels),
            out_shape=jax.ShapeDtypeStruct((6, count), F32),
            in_specs=[pl.BlockSpec(memory_space=pltpu.VMEM)] * 3,
            out_specs=pl.BlockSpec(memory_space=pltpu.VMEM),
            scratch_shapes=[
                rows((STEPS, ring, 8, count), F32),
                rows((count, 128), BF16),
                rows((count, 128), BF16),
                rows((16, count), BF16),
                rows((16, count), BF16),
                rows((2, 48, count), BF16),
                rows((STEPS + 1, 3, count), F32),
                rows((STEPS, 3, count), F32),
                rows((STEPS + 4, 3, count), F32),
                rows((STEPS + 3, 3, count), F32),
                rows((STEPS + 3, 3, count), F32),
                rows((3, count), F32),
                rows((16, count), F32),
                rows((8, count), F32),
                rows((8, count), F32),
                dma((STEPS, ring)),
                dma((STEPS, ring)),
                dma((2, STEPS)),
                dma((2, STEPS)),
                dma((2,)),
                dma((2,)),
            ],
            compiler_params=pltpu.CompilerParams(
                collective_id=0, has_side_effects=True, vmem_limit_bytes=48 * 1024 * 1024
            ),
        )(state[0], history[0], masses[None, :])
        return result[None]

    placed = (P("level", None, "body"), P("level", None, None, "body"), P("body"))
    return jax.shard_map(
        on_device, mesh=mesh, in_specs=placed, out_specs=P("level", None, "body"), check_vma=False
    )
```

```python
import functools

import jax
import jax.numpy as jnp
from jax import lax
from jax.experimental import pallas as pl
from jax.experimental.pallas import tpu as pltpu
from jax.sharding import PartitionSpec as P

STEPS = 4
SOFTEN = 0.05
DELTA = 0.05
COUPLING = 512.0
BF16 = jnp.bfloat16
F8 = jnp.float8_e4m3fn
F32 = jnp.float32
TILE = 256
SIDES = 2
LEAD = 3
SPAN = 8.0
SQUARE_SPAN = 4096.0


def split_in_three(x):
    high = x.astype(BF16).astype(F32)
    rest = x - high
    middle = rest.astype(BF16).astype(F32)
    return high, middle, rest - middle


def corrected(current, force, past, lower, level):
    oldest, middle, newest = past
    quadrature = (
        oldest / 24.0 - 5.0 * middle / 24.0 + 19.0 * newest / 24.0 + 9.0 * lower / 24.0
    )
    return jnp.where(
        level == 0,
        current + DELTA * force,
        current + DELTA * (force - newest) + DELTA * quadrature,
    )


def kernel(ring, levels, *refs):
    count = refs[0].shape[-1]
    accumulators = []
    for side in range(SIDES):
        accumulators += [pltpu.ACC(side)((TILE, TILE), F32)] * 2
        accumulators += [pltpu.ACC(side)((16, TILE), F32)] * (count // TILE)

    def scoped(*held):
        each = len(held) // SIDES
        sides = (held[:each], held[each:])
        window(ring, levels, [s[:2] for s in sides], [s[2:] for s in sides], *refs)

    pl.run_scoped(scoped, *accumulators)


def window(
    ring, levels, far, near, state, history, masses, out,
    blocks, left_even, left_odd, right_even, right_odd, target_pieces, vel, acc, hist_v, hist_a, low_hist,
    sums, target_rows, source_rows,
    pos_send, pos_recv, acc_send, acc_recv, low_send, low_recv, load_sem, told,
):
    count = state.shape[-1]
    tiles = count // TILE
    level = lax.axis_index("level")
    me = lax.axis_index("body")
    total_turns = STEPS * ring
    left = (left_even, left_odd)
    right = (right_even, right_odd)

    def above(distance):
        return lax.rem(level + distance, levels)

    line = ring // 2
    rank = me // 2
    half = lax.rem(me, 2)
    edge = jnp.minimum(rank, line - 1 - rank)
    near_count = 1 + 2 * (rank > 0).astype(jnp.int32) + 2 * (rank < line - 1).astype(jnp.int32)

    def peer(k):
        q = k // 2
        swing = rank + (q + 1) // 2 * (2 * lax.rem(q, 2) - 1)
        beyond = jnp.where(rank <= line - 1 - rank, q, line - 1 - q)
        other = jnp.where(q <= 2 * edge, swing, beyond)
        return 2 * other + lax.rem(half + k, 2)

    def pos_copy(step, k):
        return pltpu.make_async_remote_copy(
            src_ref=blocks.at[step, me, 0:4],
            dst_ref=blocks.at[step, me, 0:4],
            send_sem=pos_send.at[step, k],
            recv_sem=pos_recv.at[step, me],
            device_id=(level, peer(k)),
            device_id_type=pl.DeviceIdType.MESH,
        )

    def pos_arrival(step, owner):
        return pltpu.make_async_remote_copy(
            src_ref=blocks.at[step, owner, 0:4],
            dst_ref=blocks.at[step, owner, 0:4],
            send_sem=pos_send.at[step, 0],
            recv_sem=pos_recv.at[step, owner],
            device_id=(level, owner),
            device_id_type=pl.DeviceIdType.MESH,
        )

    def acc_copy(step, distance):
        target = (hist_a, low_hist)[distance - 1]
        return pltpu.make_async_remote_copy(
            src_ref=acc.at[step],
            dst_ref=target.at[step + 3],
            send_sem=acc_send.at[distance - 1, step],
            recv_sem=acc_recv.at[distance - 1, step],
            device_id=(above(distance), me),
            device_id_type=pl.DeviceIdType.MESH,
        )

    def low_copy():
        return pltpu.make_async_remote_copy(
            src_ref=vel.at[0],
            dst_ref=hist_v.at[3],
            send_sem=low_send.at[0],
            recv_sem=low_recv.at[0],
            device_id=(above(1), me),
            device_id_type=pl.DeviceIdType.MESH,
        )

    def low_hist_copy():
        return pltpu.make_async_remote_copy(
            src_ref=hist_a.at[0:3],
            dst_ref=low_hist.at[0:3],
            send_sem=low_send.at[1],
            recv_sem=low_recv.at[1],
            device_id=(above(1), me),
            device_id_type=pl.DeviceIdType.MESH,
        )

    def broadcast(step, first=1, last=ring):
        def one(k, carry):
            pos_copy(step, k).start()
            return carry
        lax.fori_loop(first, last, one, 0)

    barrier = pltpu.get_barrier_semaphore()

    def greet(k, carry):
        pl.semaphore_signal(
            barrier, inc=1, device_id=(level, peer(k)), device_id_type=pl.DeviceIdType.MESH
        )
        return carry

    lax.fori_loop(1, near_count + 1, greet, 0)

    def greet_level(distance, carry):
        pl.semaphore_signal(
            barrier, inc=1, device_id=(above(distance), me), device_id_type=pl.DeviceIdType.MESH
        )
        return carry

    lax.fori_loop(1, levels, greet_level, 0)

    loads = [(state.at[c], blocks.at[0, me, c:c + 1]) for c in range(3)]
    loads += [(masses, blocks.at[0, me, 3:4])]
    early = len(loads)
    loads += [(state.at[3 + c], vel.at[0, c:c + 1]) for c in range(3)]
    for k in range(3):
        loads += [(history.at[k, c], hist_v.at[k, c:c + 1]) for c in range(3)]
        loads += [(history.at[k, 3 + c], hist_a.at[k, c:c + 1]) for c in range(3)]
    loads = [
        pltpu.make_async_copy(source, target, load_sem.at[n])
        for n, (source, target) in enumerate(loads)
    ]
    for load in loads:
        load.start()

    def next_position(step):
        past = (hist_v[step], hist_v[step + 1], hist_v[step + 2])
        held = blocks[step, me, 0:3]
        return corrected(held, vel[step], past, hist_v[step + 3], level)

    def next_velocity(step):
        acc_copy(step, 1).wait_recv()
        past = (hist_a[step], hist_a[step + 1], hist_a[step + 2])
        vel[step + 1] = corrected(vel[step], acc[step], past, hist_a[step + 3], level)

    def next_low_velocity(step):
        acc_copy(step, 2).wait_recv()
        past = (low_hist[step], low_hist[step + 1], low_hist[step + 2])
        hist_v[step + 4] = corrected(
            hist_v[step + 3], hist_a[step + 3], past, low_hist[step + 3], level - 1
        )

    def publish(step):
        blocks[step, me, 0:3] = next_position(step - 1)
        blocks[step, me, 3:4] = blocks[0, me, 3:4]
        prepare_targets(step)

    def augmented(step, owner):
        p = blocks[step, owner, 0:3]
        return p, jnp.sum(p * p, axis=0, keepdims=True), blocks[step, owner, 3:4]

    def prepare_targets(step):
        p, square, _ = augmented(step, me)
        target_rows[0:3] = (-2.0 / SPAN) * p
        target_rows[4:5] = (square + SOFTEN) * (1.0 / SQUARE_SPAN)
        rest = target_rows[...]
        pieces = []
        for _ in range(8):
            pieces.append(rest.astype(F8).astype(F32))
            rest = (rest - pieces[-1]) * 16.0
        pieces = pieces + pieces[:4] + pieces[:2] + [jnp.zeros((16, count), F32)]
        target_pieces[lax.rem(step, 2)] = jnp.concatenate(pieces, axis=0).astype(F8)

    def prepare_sources(slot, step, owner):
        p, square, mass = augmented(step, owner)
        source_rows[0:3] = p * SPAN
        source_rows[3:4] = square
        source = source_rows[...]
        high, middle, low = split_in_three(source)
        high, middle, low = [
            jnp.concatenate([part, part * 0.0625], axis=0).astype(BF16)
            for part in (high, middle, low)
        ]
        steps = [jnp.array(2.0 ** -(8 * k), BF16) for k in range(4)]
        rows = [high] + [high * by for by in steps[1:]] + [middle, middle * steps[1], low]
        rows.append(jnp.zeros((16, count), BF16))
        left[slot][...] = jnp.concatenate(rows, axis=0).T
        moments = source * mass
        coarse = moments.astype(BF16).astype(F32)
        right[slot][...] = jnp.concatenate([coarse, moments - coarse], axis=0).astype(BF16)

    rounds = [(j, i) for j in range(tiles) for i in range(tiles)]
    registers = [0] * SIDES

    def stage(value, side):
        register = registers[side]
        registers[side] = 1 - register
        pltpu.matmul_push_rhs(value, staging_register=register, mxu_index=side)
        return register

    def buffer(index):
        return far[index % SIDES][(index // SIDES) % 2]

    def distances(index, slot, step):
        j, i = rounds[index]
        at = i * TILE
        pieces = target_pieces[lax.rem(step, 2), :, at:at + TILE]
        pieces = jnp.concatenate([pieces, jnp.zeros((TILE // 2, TILE), F8)], axis=0)
        lhs = left[slot][j * TILE:(j + 1) * TILE]
        lhs = jnp.concatenate([lhs, jnp.zeros((TILE, 128), BF16)], axis=1)
        register = stage(pieces, index % SIDES)
        pltpu.matmul_acc_lhs(buffer(index), lhs, load_staged_rhs=register)

    def pulls(index, slot):
        j, i = rounds[index]
        part = right[slot][:, j * TILE:(j + 1) * TILE]
        inverse = lax.rsqrt(pltpu.matmul_pop(buffer(index)))
        weight = inverse * inverse * inverse
        weight_high = weight.astype(BF16)
        weight_low = weight - weight_high.astype(F32)
        for side, piece in enumerate((weight_high, weight_low)):
            register = stage(piece, side)
            pltpu.matmul_acc_lhs(near[side][i], part, load_staged_rhs=register)

    def add_block(slot, step, next_step):
        for index in range(len(rounds)):
            ahead = index + LEAD
            if ahead < len(rounds):
                distances(ahead, slot, step)
            elif next_step is not None:
                distances(ahead - len(rounds), 1 - slot, next_step)
            pulls(index, slot)

    for side in range(SIDES):
        for used in far[side] + near[side]:
            pltpu.matmul_pop(used)

    def finish(step):
        for i in range(tiles):
            high = pltpu.matmul_pop(near[0][i])
            sums[:, i * TILE:(i + 1) * TILE] = high + pltpu.matmul_pop(near[1][i])
        total = sums[0:8] + sums[8:16]
        own = blocks[step, me, 0:3]
        acc[step] = (total[0:3] * (1.0 / SPAN) - own * (total[4:5] * (1.0 / SQUARE_SPAN))) * (
            COUPLING / (count * ring)
        )

    target_rows[...] = jnp.zeros((8, count), F32)
    target_rows[3:4] = jnp.ones((1, count), F32)
    source_rows[...] = jnp.zeros((8, count), F32)
    source_rows[4:5] = jnp.full((1, count), SQUARE_SPAN, F32)
    for load in loads[:early]:
        load.wait()
    prepare_targets(0)
    prepare_sources(0, 0, me)
    for index in range(LEAD):
        distances(index, 0, 0)
    for load in loads[early:]:
        load.wait()
    pl.semaphore_wait(barrier, near_count + levels - 1)
    broadcast(0, 1, near_count + 1)
    low_copy().start()
    low_hist_copy().start()

    def tell():
        for side, step in enumerate((2, -2)):
            @pl.when((rank < line - 1) if step > 0 else (rank > 0))
            def _():
                pl.semaphore_signal(
                    told.at[side], inc=1, device_id=(level, me + step),
                    device_id_type=pl.DeviceIdType.MESH,
                )

    def hear():
        for side, step in enumerate((2, -2)):
            @pl.when((rank > 0) if step > 0 else (rank < line - 1))
            def _():
                pl.semaphore_wait(told.at[side], 1)

    tell()
    add_block(0, 0, None)
    hear()

    def relay(_, carry):
        tell()
        hear()
        return carry

    lax.fori_loop(0, line - 3, relay, 0)
    broadcast(0, near_count + 1, ring)
    first = peer(1)
    pos_arrival(0, first).wait_recv()
    prepare_sources(1, 0, first)
    for index in range(LEAD):
        distances(index, 1, 0)

    def one_turn(turn, slot):
        step = turn // ring
        k = lax.rem(turn, ring)
        after = lax.rem(turn + 1, total_turns)
        next_step = after // ring
        next_k = lax.rem(after, ring)

        if slot == 1:
            @pl.when((k == 1) & (step > 0))
            def _():
                acc_copy(step - 1, 1).start()
                acc_copy(step - 1, 2).start()

            @pl.when((k == 3) & (step == 0))
            def _():
                low_copy().wait_recv()
                publish(1)

            @pl.when((k == 5) & (step > 0) & (step < STEPS - 1))
            def _():
                broadcast(step + 1)
        else:
            @pl.when((k == 4) & (step == 0))
            def _():
                low_hist_copy().wait_recv()
                broadcast(1)

            @pl.when((k == 4) & (step > 0))
            def _():
                next_velocity(step - 1)
                next_low_velocity(step - 1)

                @pl.when(step < STEPS - 1)
                def _():
                    publish(step + 1)

        @pl.when(next_k > 0)
        def _():
            pos_arrival(next_step, peer(next_k)).wait_recv()

        prepare_sources(1 - slot, next_step, peer(next_k))
        add_block(slot, step, next_step)

        if slot == 1:
            @pl.when(k == ring - 1)
            def _():
                finish(step)

    def two_turns(pair, carry):
        one_turn(2 * pair + 1, 1)
        one_turn(2 * pair + 2, 0)
        return carry

    lax.fori_loop(0, total_turns // 2 - 1, two_turns, 0)
    one_turn(total_turns - 1, 1)
    for index in range(LEAD):
        pltpu.matmul_pop(buffer(index))
    acc_copy(STEPS - 1, 1).start()
    moved = next_position(STEPS - 1)
    for c in range(3):
        out[c] = moved[c:c + 1]
    next_velocity(STEPS - 1)
    for c in range(3):
        out[3 + c] = vel[STEPS, c:c + 1]

    def drain(step, carry):
        def one(k, inner):
            pos_copy(step, k).wait_send()
            return inner
        lax.fori_loop(1, ring, one, 0)
        acc_copy(step, 1).wait_send()

        @pl.when(step < STEPS - 1)
        def _():
            acc_copy(step, 2).wait_send()

        return carry

    lax.fori_loop(0, STEPS, drain, 0)
    low_copy().wait_send()
    low_hist_copy().wait_send()


def solution(mesh):
    ring = mesh.shape["body"]
    levels = mesh.shape["level"]

    def on_device(state, history, masses):
        count = state.shape[2]
        dma = pltpu.SemaphoreType.DMA
        rows = pltpu.VMEM
        result = pl.pallas_call(
            functools.partial(kernel, ring, levels),
            out_shape=jax.ShapeDtypeStruct((6, 1, count), F32),
            in_specs=[pl.BlockSpec(memory_space=pltpu.HBM)] * 3,
            out_specs=pl.BlockSpec(memory_space=pltpu.VMEM),
            scratch_shapes=[
                rows((STEPS, ring, 8, count), F32),
                rows((count, 128), BF16),
                rows((count, 128), BF16),
                rows((16, count), BF16),
                rows((16, count), BF16),
                rows((2, 128, count), F8),
                rows((STEPS + 1, 3, count), F32),
                rows((STEPS, 3, count), F32),
                rows((STEPS + 4, 3, count), F32),
                rows((STEPS + 3, 3, count), F32),
                rows((STEPS + 3, 3, count), F32),
                rows((16, count), F32),
                rows((8, count), F32),
                rows((8, count), F32),
                dma((STEPS, ring)),
                dma((STEPS, ring)),
                dma((2, STEPS)),
                dma((2, STEPS)),
                dma((2,)),
                dma((2,)),
                dma((25,)),
                pltpu.SemaphoreType.REGULAR((2,)),
            ],
            compiler_params=pltpu.CompilerParams(
                collective_id=0, has_side_effects=True, vmem_limit_bytes=60 * 1024 * 1024
            ),
        )(
            state.reshape(6, 1, count), history.reshape(3, 6, 1, count), masses.reshape(1, count)
        )
        return result.reshape(1, 6, count)

    placed = (P("level", None, "body"), P("level", None, None, "body"), P("body"))
    return jax.shard_map(
        on_device, mesh=mesh, in_specs=placed, out_specs=P("level", None, "body"), check_vma=False
    )
```

```python
import functools

import jax
import jax.numpy as jnp
from jax import lax
from jax.experimental import pallas as pl
from jax.experimental.pallas import tpu as pltpu
from jax.sharding import PartitionSpec as P

STEPS = 4
SOFTEN = 0.05
DELTA = 0.05
COUPLING = 512.0
BF16 = jnp.bfloat16
F8 = jnp.float8_e4m3fn
F32 = jnp.float32
TILE = 256
SIDES = 2
LEAD = 3
SPAN = 8.0
SQUARE_SPAN = 4096.0


def split_in_three(x):
    high = x.astype(BF16).astype(F32)
    rest = x - high
    middle = rest.astype(BF16).astype(F32)
    return high, middle, rest - middle


def corrected(current, force, past, lower, level):
    oldest, middle, newest = past
    quadrature = (
        oldest / 24.0 - 5.0 * middle / 24.0 + 19.0 * newest / 24.0 + 9.0 * lower / 24.0
    )
    return jnp.where(
        level == 0,
        current + DELTA * force,
        current + DELTA * (force - newest) + DELTA * quadrature,
    )


def kernel(ring, levels, *refs):
    count = refs[0].shape[-1]
    accumulators = []
    for side in range(SIDES):
        accumulators += [pltpu.ACC(side)((TILE, TILE), F32)] * 2
        accumulators += [pltpu.ACC(side)((16, TILE), F32)] * (count // TILE)

    def scoped(*held):
        each = len(held) // SIDES
        sides = (held[:each], held[each:])
        window(ring, levels, [s[:2] for s in sides], [s[2:] for s in sides], *refs)

    pl.run_scoped(scoped, *accumulators)


def window(
    ring, levels, far, near, state, history, masses, out,
    blocks, left_even, left_odd, right_even, right_odd, target_pieces, vel, acc, hist_v, hist_a, low_hist,
    sums, target_rows, source_rows,
    pos_send, pos_recv, acc_send, acc_recv, low_send, low_recv, load_sem, told,
):
    count = state.shape[-1]
    tiles = count // TILE
    level = lax.axis_index("level")
    me = lax.axis_index("body")
    total_turns = STEPS * ring
    left = (left_even, left_odd)
    right = (right_even, right_odd)

    def above(distance):
        return lax.rem(level + distance, levels)

    line = ring // 2
    rank = me // 2
    half = lax.rem(me, 2)
    edge = jnp.minimum(rank, line - 1 - rank)

    def within(pairs):
        return 1 + 2 * (jnp.minimum(rank, pairs) + jnp.minimum(line - 1 - rank, pairs))

    near_count = within(1)

    def peer(k):
        q = k // 2
        swing = rank + (q + 1) // 2 * (2 * lax.rem(q, 2) - 1)
        beyond = jnp.where(rank <= line - 1 - rank, q, line - 1 - q)
        other = jnp.where(q <= 2 * edge, swing, beyond)
        return 2 * other + lax.rem(half + k, 2)

    def pos_copy(step, k):
        return pltpu.make_async_remote_copy(
            src_ref=blocks.at[step, me, 0:4],
            dst_ref=blocks.at[step, me, 0:4],
            send_sem=pos_send.at[step, k],
            recv_sem=pos_recv.at[step, me],
            device_id=(level, peer(k)),
            device_id_type=pl.DeviceIdType.MESH,
        )

    def pos_arrival(step, owner):
        return pltpu.make_async_remote_copy(
            src_ref=blocks.at[step, owner, 0:4],
            dst_ref=blocks.at[step, owner, 0:4],
            send_sem=pos_send.at[step, 0],
            recv_sem=pos_recv.at[step, owner],
            device_id=(level, owner),
            device_id_type=pl.DeviceIdType.MESH,
        )

    def acc_copy(step, distance):
        target = (hist_a, low_hist)[distance - 1]
        return pltpu.make_async_remote_copy(
            src_ref=acc.at[step],
            dst_ref=target.at[step + 3],
            send_sem=acc_send.at[distance - 1, step],
            recv_sem=acc_recv.at[distance - 1, step],
            device_id=(above(distance), me),
            device_id_type=pl.DeviceIdType.MESH,
        )

    def low_copy():
        return pltpu.make_async_remote_copy(
            src_ref=vel.at[0],
            dst_ref=hist_v.at[3],
            send_sem=low_send.at[0],
            recv_sem=low_recv.at[0],
            device_id=(above(1), me),
            device_id_type=pl.DeviceIdType.MESH,
        )

    def low_hist_copy():
        return pltpu.make_async_remote_copy(
            src_ref=hist_a.at[0:3],
            dst_ref=low_hist.at[0:3],
            send_sem=low_send.at[1],
            recv_sem=low_recv.at[1],
            device_id=(above(1), me),
            device_id_type=pl.DeviceIdType.MESH,
        )

    def broadcast(step, first=1, last=ring):
        def one(k, carry):
            pos_copy(step, k).start()
            return carry
        lax.fori_loop(first, last, one, 0)

    barrier = pltpu.get_barrier_semaphore()

    def greet(k, carry):
        pl.semaphore_signal(
            barrier, inc=1, device_id=(level, peer(k)), device_id_type=pl.DeviceIdType.MESH
        )
        return carry

    lax.fori_loop(1, near_count + 1, greet, 0)

    def greet_level(distance, carry):
        pl.semaphore_signal(
            barrier, inc=1, device_id=(above(distance), me), device_id_type=pl.DeviceIdType.MESH
        )
        return carry

    lax.fori_loop(1, levels, greet_level, 0)

    loads = [(state.at[c], blocks.at[0, me, c:c + 1]) for c in range(3)]
    loads += [(masses, blocks.at[0, me, 3:4])]
    early = len(loads)
    loads += [(state.at[3 + c], vel.at[0, c:c + 1]) for c in range(3)]
    for k in range(3):
        loads += [(history.at[k, c], hist_v.at[k, c:c + 1]) for c in range(3)]
        loads += [(history.at[k, 3 + c], hist_a.at[k, c:c + 1]) for c in range(3)]
    loads = [
        pltpu.make_async_copy(source, target, load_sem.at[n])
        for n, (source, target) in enumerate(loads)
    ]
    for load in loads:
        load.start()

    def next_position(step):
        past = (hist_v[step], hist_v[step + 1], hist_v[step + 2])
        held = blocks[step, me, 0:3]
        return corrected(held, vel[step], past, hist_v[step + 3], level)

    def next_velocity(step):
        acc_copy(step, 1).wait_recv()
        past = (hist_a[step], hist_a[step + 1], hist_a[step + 2])
        vel[step + 1] = corrected(vel[step], acc[step], past, hist_a[step + 3], level)

    def next_low_velocity(step):
        acc_copy(step, 2).wait_recv()
        past = (low_hist[step], low_hist[step + 1], low_hist[step + 2])
        hist_v[step + 4] = corrected(
            hist_v[step + 3], hist_a[step + 3], past, low_hist[step + 3], level - 1
        )

    def publish(step):
        blocks[step, me, 0:3] = next_position(step - 1)
        blocks[step, me, 3:4] = blocks[0, me, 3:4]
        prepare_targets(step)

    def augmented(step, owner):
        p = blocks[step, owner, 0:3]
        return p, jnp.sum(p * p, axis=0, keepdims=True), blocks[step, owner, 3:4]

    def prepare_targets(step):
        p, square, _ = augmented(step, me)
        target_rows[0:3] = (-2.0 / SPAN) * p
        target_rows[4:5] = (square + SOFTEN) * (1.0 / SQUARE_SPAN)
        rest = target_rows[...]
        pieces = []
        for _ in range(8):
            pieces.append(rest.astype(F8).astype(F32))
            rest = (rest - pieces[-1]) * 16.0
        pieces = pieces + pieces[:4] + pieces[:2] + [jnp.zeros((16, count), F32)]
        target_pieces[lax.rem(step, 2)] = jnp.concatenate(pieces, axis=0).astype(F8)

    def prepare_sources(slot, step, owner):
        p, square, mass = augmented(step, owner)
        source_rows[0:3] = p * SPAN
        source_rows[3:4] = square
        source = source_rows[...]
        high, middle, low = split_in_three(source)
        high, middle, low = [
            jnp.concatenate([part, part * 0.0625], axis=0).astype(BF16)
            for part in (high, middle, low)
        ]
        steps = [jnp.array(2.0 ** -(8 * k), BF16) for k in range(4)]
        rows = [high] + [high * by for by in steps[1:]] + [middle, middle * steps[1], low]
        rows.append(jnp.zeros((16, count), BF16))
        left[slot][...] = jnp.concatenate(rows, axis=0).T
        moments = source * mass
        coarse = moments.astype(BF16).astype(F32)
        right[slot][...] = jnp.concatenate([coarse, moments - coarse], axis=0).astype(BF16)

    rounds = [(j, i) for j in range(tiles) for i in range(tiles)]
    registers = [0] * SIDES

    def stage(value, side):
        register = registers[side]
        registers[side] = 1 - register
        pltpu.matmul_push_rhs(value, staging_register=register, mxu_index=side)
        return register

    def buffer(index):
        return far[index % SIDES][(index // SIDES) % 2]

    def distances(index, slot, step):
        j, i = rounds[index]
        at = i * TILE
        pieces = target_pieces[lax.rem(step, 2), :, at:at + TILE]
        pieces = jnp.concatenate([pieces, jnp.zeros((TILE // 2, TILE), F8)], axis=0)
        lhs = left[slot][j * TILE:(j + 1) * TILE]
        lhs = jnp.concatenate([lhs, jnp.zeros((TILE, 128), BF16)], axis=1)
        register = stage(pieces, index % SIDES)
        pltpu.matmul_acc_lhs(buffer(index), lhs, load_staged_rhs=register)

    def pulls(index, slot):
        j, i = rounds[index]
        part = right[slot][:, j * TILE:(j + 1) * TILE]
        inverse = lax.rsqrt(pltpu.matmul_pop(buffer(index)))
        weight = inverse * inverse * inverse
        weight_high = weight.astype(BF16)
        weight_low = weight - weight_high.astype(F32)
        for side, piece in enumerate((weight_high, weight_low)):
            register = stage(piece, side)
            pltpu.matmul_acc_lhs(near[side][i], part, load_staged_rhs=register)

    def add_block(slot, step, next_step, first=0, last=len(rounds)):
        for index in range(first, last):
            ahead = index + LEAD
            if ahead < len(rounds):
                distances(ahead, slot, step)
            elif next_step is not None:
                distances(ahead - len(rounds), 1 - slot, next_step)
            pulls(index, slot)

    for side in range(SIDES):
        for used in far[side] + near[side]:
            pltpu.matmul_pop(used)

    def finish(step):
        for i in range(tiles):
            high = pltpu.matmul_pop(near[0][i])
            sums[:, i * TILE:(i + 1) * TILE] = high + pltpu.matmul_pop(near[1][i])
        total = sums[0:8] + sums[8:16]
        own = blocks[step, me, 0:3]
        acc[step] = (total[0:3] * (1.0 / SPAN) - own * (total[4:5] * (1.0 / SQUARE_SPAN))) * (
            COUPLING / (count * ring)
        )

    target_rows[...] = jnp.zeros((8, count), F32)
    target_rows[3:4] = jnp.ones((1, count), F32)
    source_rows[...] = jnp.zeros((8, count), F32)
    source_rows[4:5] = jnp.full((1, count), SQUARE_SPAN, F32)
    def tell():
        for side, step in enumerate((2, -2)):
            @pl.when((rank < line - 1) if step > 0 else (rank > 0))
            def _():
                pl.semaphore_signal(
                    told.at[side], inc=1, device_id=(level, me + step),
                    device_id_type=pl.DeviceIdType.MESH,
                )

    def hear():
        for side, step in enumerate((2, -2)):
            @pl.when((rank > 0) if step > 0 else (rank < line - 1))
            def _():
                pl.semaphore_wait(told.at[side], 1)

    for load in loads[:early]:
        load.wait()
    pl.semaphore_wait(barrier, near_count + levels - 1)
    broadcast(0, 1, near_count + 1)
    tell()
    for load in loads[early:]:
        load.wait()
    low_copy().start()
    low_hist_copy().start()
    prepare_targets(0)
    prepare_sources(0, 0, me)
    for index in range(LEAD):
        distances(index, 0, 0)
    middle = len(rounds) // 2
    add_block(0, 0, None, 0, middle)
    hear()
    broadcast(0, near_count + 1, within(2) + 1)
    tell()
    add_block(0, 0, None, middle)
    hear()

    def relay(_, carry):
        tell()
        hear()
        return carry

    lax.fori_loop(0, line - 4, relay, 0)
    broadcast(0, within(2) + 1, ring)
    first = peer(1)
    pos_arrival(0, first).wait_recv()
    prepare_sources(1, 0, first)
    for index in range(LEAD):
        distances(index, 1, 0)

    def one_turn(turn, slot, last=False):
        step = turn // ring
        k = lax.rem(turn, ring)
        after = lax.rem(turn + 1, total_turns)
        next_step = after // ring
        next_k = lax.rem(after, ring)

        if slot == 0:
            @pl.when((k == 0) & (step > 0))
            def _():
                acc_copy(step - 1, 1).start()
                acc_copy(step - 1, 2).start()

            @pl.when((k == 4) & (step < STEPS - 1))
            def _():
                @pl.when(step == 0)
                def _():
                    low_hist_copy().wait_recv()

                broadcast(step + 1)
        else:
            @pl.when(k == 3)
            def _():
                @pl.when(step == 0)
                def _():
                    low_copy().wait_recv()

                @pl.when(step > 0)
                def _():
                    next_velocity(step - 1)
                    next_low_velocity(step - 1)

                @pl.when(step < STEPS - 1)
                def _():
                    publish(step + 1)

        if last:
            add_block(slot, step, None)
            finish(step)
            return

        @pl.when(next_k > 0)
        def _():
            pos_arrival(next_step, peer(next_k)).wait_recv()

        prepare_sources(1 - slot, next_step, peer(next_k))
        add_block(slot, step, next_step)

        if slot == 1:
            @pl.when(k == ring - 1)
            def _():
                finish(step)

    def two_turns(pair, carry):
        one_turn(2 * pair + 1, 1)
        one_turn(2 * pair + 2, 0)
        return carry

    lax.fori_loop(0, total_turns // 2 - 1, two_turns, 0)
    one_turn(total_turns - 1, 1, last=True)
    acc_copy(STEPS - 1, 1).start()
    moved = next_position(STEPS - 1)
    for c in range(3):
        out[c] = moved[c:c + 1]
    next_velocity(STEPS - 1)
    for c in range(3):
        out[3 + c] = vel[STEPS, c:c + 1]

    def drain(step, carry):
        def one(k, inner):
            pos_copy(step, k).wait_send()
            return inner
        lax.fori_loop(1, ring, one, 0)
        acc_copy(step, 1).wait_send()

        @pl.when(step < STEPS - 1)
        def _():
            acc_copy(step, 2).wait_send()

        return carry

    lax.fori_loop(0, STEPS, drain, 0)
    low_copy().wait_send()
    low_hist_copy().wait_send()


def solution(mesh):
    ring = mesh.shape["body"]
    levels = mesh.shape["level"]

    def on_device(state, history, masses):
        count = state.shape[2]
        dma = pltpu.SemaphoreType.DMA
        rows = pltpu.VMEM
        result = pl.pallas_call(
            functools.partial(kernel, ring, levels),
            out_shape=pltpu.VMEM((6, 1, count), F32),
            in_specs=[pl.BlockSpec(memory_space=pltpu.HBM)] * 3,
            out_specs=pl.BlockSpec(memory_space=pltpu.VMEM),
            scratch_shapes=[
                rows((STEPS, ring, 8, count), F32),
                rows((count, 128), BF16),
                rows((count, 128), BF16),
                rows((16, count), BF16),
                rows((16, count), BF16),
                rows((2, 128, count), F8),
                rows((STEPS + 1, 3, count), F32),
                rows((STEPS, 3, count), F32),
                rows((STEPS + 4, 3, count), F32),
                rows((STEPS + 3, 3, count), F32),
                rows((STEPS + 3, 3, count), F32),
                rows((16, count), F32),
                rows((8, count), F32),
                rows((8, count), F32),
                dma((STEPS, ring)),
                dma((STEPS, ring)),
                dma((2, STEPS)),
                dma((2, STEPS)),
                dma((2,)),
                dma((2,)),
                dma((25,)),
                pltpu.SemaphoreType.REGULAR((2,)),
            ],
            compiler_params=pltpu.CompilerParams(
                collective_id=0, has_side_effects=True, vmem_limit_bytes=60 * 1024 * 1024
            ),
        )(
            state.reshape(6, 1, count), history.reshape(3, 6, 1, count), masses.reshape(1, count)
        )
        return result.reshape(1, 6, count)

    placed = (P("level", None, "body"), P("level", None, None, "body"), P("body"))
    return jax.shard_map(
        on_device, mesh=mesh, in_specs=placed, out_specs=P("level", None, "body"), check_vma=False
    )
```

```python
import functools

import jax
import jax.numpy as jnp
from jax import lax
from jax.experimental import pallas as pl
from jax.experimental.pallas import tpu as pltpu
from jax.sharding import PartitionSpec as P

STEPS = 4
SOFTEN = 0.05
DELTA = 0.05
COUPLING = 512.0
BF16 = jnp.bfloat16
F8 = jnp.float8_e4m3fn
F32 = jnp.float32
TILE = 256
SIDES = 2
LEAD = 3
SPAN = 8.0
SQUARE_SPAN = 4096.0


def split_in_three(x):
    high = x.astype(BF16).astype(F32)
    rest = x - high
    middle = rest.astype(BF16).astype(F32)
    return high, middle, rest - middle


def corrected(current, force, past, lower, level):
    oldest, middle, newest = past
    quadrature = (
        oldest / 24.0 - 5.0 * middle / 24.0 + 19.0 * newest / 24.0 + 9.0 * lower / 24.0
    )
    return jnp.where(
        level == 0,
        current + DELTA * force,
        current + DELTA * (force - newest) + DELTA * quadrature,
    )


def kernel(ring, levels, *refs):
    count = refs[0].shape[-1]
    accumulators = []
    for side in range(SIDES):
        accumulators += [pltpu.ACC(side)((TILE, TILE), F32)] * 2
        accumulators += [pltpu.ACC(side)((16, TILE), F32)] * (count // TILE)

    def scoped(*held):
        each = len(held) // SIDES
        sides = (held[:each], held[each:])
        window(ring, levels, [s[:2] for s in sides], [s[2:] for s in sides], *refs)

    pl.run_scoped(scoped, *accumulators)


def window(
    ring, levels, far, near, state, history, masses, out,
    blocks, left_even, left_odd, right_even, right_odd, target_pieces, vel, acc, hist_v, hist_a, low_hist,
    sums, target_rows, source_rows,
    pos_send, pos_recv, acc_send, acc_recv, low_send, low_recv, load_sem, told,
):
    count = state.shape[-1]
    tiles = count // TILE
    level = lax.axis_index("level")
    me = lax.axis_index("body")
    total_turns = STEPS * ring
    left = (left_even, left_odd)
    right = (right_even, right_odd)

    def above(distance):
        return lax.rem(level + distance, levels)

    line = ring // 2
    rank = me // 2
    half = lax.rem(me, 2)
    edge = jnp.minimum(rank, line - 1 - rank)

    def within(pairs):
        return 1 + 2 * (jnp.minimum(rank, pairs) + jnp.minimum(line - 1 - rank, pairs))

    near_count = within(1)

    def peer(k):
        q = k // 2
        swing = rank + (q + 1) // 2 * (2 * lax.rem(q, 2) - 1)
        beyond = jnp.where(rank <= line - 1 - rank, q, line - 1 - q)
        other = jnp.where(q <= 2 * edge, swing, beyond)
        return 2 * other + lax.rem(half + k, 2)

    def pos_copy(step, k):
        return pltpu.make_async_remote_copy(
            src_ref=blocks.at[step, me, 0:4],
            dst_ref=blocks.at[step, me, 0:4],
            send_sem=pos_send.at[step],
            recv_sem=pos_recv.at[step, me],
            device_id=(level, peer(k)),
            device_id_type=pl.DeviceIdType.MESH,
        )

    def pos_arrival(step, owner):
        return pltpu.make_async_remote_copy(
            src_ref=blocks.at[step, owner, 0:4],
            dst_ref=blocks.at[step, owner, 0:4],
            send_sem=pos_send.at[step],
            recv_sem=pos_recv.at[step, owner],
            device_id=(level, owner),
            device_id_type=pl.DeviceIdType.MESH,
        )

    def acc_copy(step, distance):
        target = (hist_a, low_hist)[distance - 1]
        return pltpu.make_async_remote_copy(
            src_ref=acc.at[step],
            dst_ref=target.at[step + 3],
            send_sem=acc_send.at[distance - 1, step],
            recv_sem=acc_recv.at[distance - 1, step],
            device_id=(above(distance), me),
            device_id_type=pl.DeviceIdType.MESH,
        )

    def low_copy():
        return pltpu.make_async_remote_copy(
            src_ref=vel.at[0],
            dst_ref=hist_v.at[3],
            send_sem=low_send.at[0],
            recv_sem=low_recv.at[0],
            device_id=(above(1), me),
            device_id_type=pl.DeviceIdType.MESH,
        )

    def low_hist_copy():
        return pltpu.make_async_remote_copy(
            src_ref=hist_a.at[0:3],
            dst_ref=low_hist.at[0:3],
            send_sem=low_send.at[1],
            recv_sem=low_recv.at[1],
            device_id=(above(1), me),
            device_id_type=pl.DeviceIdType.MESH,
        )

    def broadcast(step, first=1, last=ring):
        def one(k, carry):
            pos_copy(step, k).start()
            return carry
        lax.fori_loop(first, last, one, 0)

    barrier = pltpu.get_barrier_semaphore()

    def greet(k, carry):
        pl.semaphore_signal(
            barrier, inc=1, device_id=(level, peer(k)), device_id_type=pl.DeviceIdType.MESH
        )
        return carry

    lax.fori_loop(1, near_count + 1, greet, 0)

    def greet_level(distance, carry):
        pl.semaphore_signal(
            barrier, inc=1, device_id=(above(distance), me), device_id_type=pl.DeviceIdType.MESH
        )
        return carry

    lax.fori_loop(1, levels, greet_level, 0)

    loads = [(state.at[c], blocks.at[0, me, c:c + 1]) for c in range(3)]
    loads += [(masses, blocks.at[0, me, 3:4])]
    early = len(loads)
    loads += [(state.at[3 + c], vel.at[0, c:c + 1]) for c in range(3)]
    for k in range(3):
        loads += [(history.at[k, c], hist_v.at[k, c:c + 1]) for c in range(3)]
        loads += [(history.at[k, 3 + c], hist_a.at[k, c:c + 1]) for c in range(3)]
    loads = [
        pltpu.make_async_copy(source, target, load_sem.at[n])
        for n, (source, target) in enumerate(loads)
    ]
    for load in loads:
        load.start()

    def next_position(step):
        past = (hist_v[step], hist_v[step + 1], hist_v[step + 2])
        held = blocks[step, me, 0:3]
        return corrected(held, vel[step], past, hist_v[step + 3], level)

    def next_velocity(step):
        acc_copy(step, 1).wait_recv()
        past = (hist_a[step], hist_a[step + 1], hist_a[step + 2])
        vel[step + 1] = corrected(vel[step], acc[step], past, hist_a[step + 3], level)

    def next_low_velocity(step):
        acc_copy(step, 2).wait_recv()
        past = (low_hist[step], low_hist[step + 1], low_hist[step + 2])
        hist_v[step + 4] = corrected(
            hist_v[step + 3], hist_a[step + 3], past, low_hist[step + 3], level - 1
        )

    def publish(step):
        blocks[step, me, 0:3] = next_position(step - 1)
        blocks[step, me, 3:4] = blocks[0, me, 3:4]
        prepare_targets(step)

    def augmented(step, owner):
        p = blocks[step, owner, 0:3]
        return p, jnp.sum(p * p, axis=0, keepdims=True), blocks[step, owner, 3:4]

    def prepare_targets(step):
        p, square, _ = augmented(step, me)
        target_rows[0:3] = (-2.0 / SPAN) * p
        target_rows[4:5] = (square + SOFTEN) * (1.0 / SQUARE_SPAN)
        rest = target_rows[...]
        pieces = []
        for _ in range(8):
            pieces.append(rest.astype(F8).astype(F32))
            rest = (rest - pieces[-1]) * 16.0
        pieces = pieces + pieces[:4] + pieces[:2] + [jnp.zeros((16, count), F32)]
        target_pieces[lax.rem(step, 2)] = jnp.concatenate(pieces, axis=0).astype(F8)

    def prepare_sources(slot, step, owner):
        p, square, mass = augmented(step, owner)
        source_rows[0:3] = p * SPAN
        source_rows[3:4] = square
        source = source_rows[...]
        high, middle, low = split_in_three(source)
        high, middle, low = [
            jnp.concatenate([part, part * 0.0625], axis=0).astype(BF16)
            for part in (high, middle, low)
        ]
        steps = [jnp.array(2.0 ** -(8 * k), BF16) for k in range(4)]
        rows = [high] + [high * by for by in steps[1:]] + [middle, middle * steps[1], low]
        rows.append(jnp.zeros((16, count), BF16))
        left[slot][...] = jnp.concatenate(rows, axis=0).T
        moments = source * mass
        coarse = moments.astype(BF16).astype(F32)
        right[slot][...] = jnp.concatenate([coarse, moments - coarse], axis=0).astype(BF16)

    rounds = [(j, i) for j in range(tiles) for i in range(tiles)]
    registers = [0] * SIDES

    def stage(value, side):
        register = registers[side]
        registers[side] = 1 - register
        pltpu.matmul_push_rhs(value, staging_register=register, mxu_index=side)
        return register

    def buffer(index):
        return far[index % SIDES][(index // SIDES) % 2]

    def distances(index, slot, step):
        j, i = rounds[index]
        at = i * TILE
        pieces = target_pieces[lax.rem(step, 2), :, at:at + TILE]
        pieces = jnp.concatenate([pieces, jnp.zeros((TILE // 2, TILE), F8)], axis=0)
        lhs = left[slot][j * TILE:(j + 1) * TILE]
        lhs = jnp.concatenate([lhs, jnp.zeros((TILE, 128), BF16)], axis=1)
        register = stage(pieces, index % SIDES)
        pltpu.matmul_acc_lhs(buffer(index), lhs, load_staged_rhs=register)

    def pulls(index, slot):
        j, i = rounds[index]
        part = right[slot][:, j * TILE:(j + 1) * TILE]
        inverse = lax.rsqrt(pltpu.matmul_pop(buffer(index)))
        weight = inverse * inverse * inverse
        weight_high = weight.astype(BF16)
        weight_low = weight - weight_high.astype(F32)
        for side, piece in enumerate((weight_high, weight_low)):
            register = stage(piece, side)
            pltpu.matmul_acc_lhs(near[side][i], part, load_staged_rhs=register)

    def add_block(slot, step, next_step, first=0, last=len(rounds)):
        for index in range(first, last):
            ahead = index + LEAD
            if ahead < len(rounds):
                distances(ahead, slot, step)
            elif next_step is not None:
                distances(ahead - len(rounds), 1 - slot, next_step)
            pulls(index, slot)

    for side in range(SIDES):
        for used in far[side] + near[side]:
            pltpu.matmul_pop(used)

    def finish(step):
        for i in range(tiles):
            high = pltpu.matmul_pop(near[0][i])
            sums[:, i * TILE:(i + 1) * TILE] = high + pltpu.matmul_pop(near[1][i])
        total = sums[0:8] + sums[8:16]
        own = blocks[step, me, 0:3]
        acc[step] = (total[0:3] * (1.0 / SPAN) - own * (total[4:5] * (1.0 / SQUARE_SPAN))) * (
            COUPLING / (count * ring)
        )

    target_rows[...] = jnp.zeros((8, count), F32)
    target_rows[3:4] = jnp.ones((1, count), F32)
    source_rows[...] = jnp.zeros((8, count), F32)
    source_rows[4:5] = jnp.full((1, count), SQUARE_SPAN, F32)
    def tell():
        for side, step in enumerate((2, -2)):
            @pl.when((rank < line - 1) if step > 0 else (rank > 0))
            def _():
                pl.semaphore_signal(
                    told.at[side], inc=1, device_id=(level, me + step),
                    device_id_type=pl.DeviceIdType.MESH,
                )

    def hear():
        for side, step in enumerate((2, -2)):
            @pl.when((rank > 0) if step > 0 else (rank < line - 1))
            def _():
                pl.semaphore_wait(told.at[side], 1)

    for load in loads[:early]:
        load.wait()
    pl.semaphore_wait(barrier, near_count + levels - 1)
    broadcast(0, 1, near_count + 1)
    tell()
    for load in loads[early:]:
        load.wait()
    low_copy().start()
    low_hist_copy().start()
    prepare_targets(0)
    prepare_sources(0, 0, me)
    for index in range(LEAD):
        distances(index, 0, 0)
    middle = len(rounds) // 2
    add_block(0, 0, None, 0, middle)
    hear()
    broadcast(0, near_count + 1, within(2) + 1)
    tell()
    add_block(0, 0, None, middle)
    hear()

    def relay(_, carry):
        tell()
        hear()
        return carry

    lax.fori_loop(0, line - 4, relay, 0)
    broadcast(0, within(2) + 1, ring)
    first = peer(1)
    pos_arrival(0, first).wait_recv()
    prepare_sources(1, 0, first)
    for index in range(LEAD):
        distances(index, 1, 0)

    def one_turn(turn, slot, last=False):
        step = turn // ring
        k = lax.rem(turn, ring)
        after = lax.rem(turn + 1, total_turns)
        next_step = after // ring
        next_k = lax.rem(after, ring)

        if slot == 0:
            @pl.when((k == 0) & (step > 0))
            def _():
                acc_copy(step - 1, 1).start()
                acc_copy(step - 1, 2).start()

            @pl.when((k == 4) & (step < STEPS - 1))
            def _():
                @pl.when(step == 0)
                def _():
                    low_hist_copy().wait_recv()

                broadcast(step + 1)
        else:
            @pl.when(k == 3)
            def _():
                @pl.when(step == 0)
                def _():
                    low_copy().wait_recv()

                @pl.when(step > 0)
                def _():
                    next_velocity(step - 1)
                    next_low_velocity(step - 1)

                @pl.when(step < STEPS - 1)
                def _():
                    publish(step + 1)

        if last:
            add_block(slot, step, None)
            finish(step)
            return

        @pl.when(next_k > 0)
        def _():
            pos_arrival(next_step, peer(next_k)).wait_recv()

        prepare_sources(1 - slot, next_step, peer(next_k))
        add_block(slot, step, next_step)

        if slot == 1:
            @pl.when(k == ring - 1)
            def _():
                finish(step)

    def two_turns(pair, carry):
        one_turn(2 * pair + 1, 1)
        one_turn(2 * pair + 2, 0)
        return carry

    lax.fori_loop(0, total_turns // 2 - 1, two_turns, 0)
    one_turn(total_turns - 1, 1, last=True)
    acc_copy(STEPS - 1, 1).start()
    moved = next_position(STEPS - 1)
    for c in range(3):
        out[c] = moved[c:c + 1]
    next_velocity(STEPS - 1)
    for c in range(3):
        out[3 + c] = vel[STEPS, c:c + 1]

    def drain(step, carry):
        pltpu.make_async_remote_copy(
            src_ref=blocks.at[step, 1:ring, 0:4],
            dst_ref=blocks.at[step, 1:ring, 0:4],
            send_sem=pos_send.at[step],
            recv_sem=pos_recv.at[step, me],
            device_id=(level, peer(1)),
            device_id_type=pl.DeviceIdType.MESH,
        ).wait_send()
        acc_copy(step, 1).wait_send()

        @pl.when(step < STEPS - 1)
        def _():
            acc_copy(step, 2).wait_send()

        return carry

    lax.fori_loop(0, STEPS, drain, 0)
    low_copy().wait_send()
    low_hist_copy().wait_send()


def solution(mesh):
    ring = mesh.shape["body"]
    levels = mesh.shape["level"]

    def on_device(state, history, masses):
        count = state.shape[2]
        dma = pltpu.SemaphoreType.DMA
        rows = pltpu.VMEM
        result = pl.pallas_call(
            functools.partial(kernel, ring, levels),
            out_shape=pltpu.VMEM((6, 1, count), F32),
            in_specs=[pl.BlockSpec(memory_space=pltpu.HBM)] * 3,
            out_specs=pl.BlockSpec(memory_space=pltpu.VMEM),
            scratch_shapes=[
                rows((STEPS, ring, 8, count), F32),
                rows((count, 128), BF16),
                rows((count, 128), BF16),
                rows((16, count), BF16),
                rows((16, count), BF16),
                rows((2, 128, count), F8),
                rows((STEPS + 1, 3, count), F32),
                rows((STEPS, 3, count), F32),
                rows((STEPS + 4, 3, count), F32),
                rows((STEPS + 3, 3, count), F32),
                rows((STEPS + 3, 3, count), F32),
                rows((16, count), F32),
                rows((8, count), F32),
                rows((8, count), F32),
                dma((STEPS,)),
                dma((STEPS, ring)),
                dma((2, STEPS)),
                dma((2, STEPS)),
                dma((2,)),
                dma((2,)),
                dma((25,)),
                pltpu.SemaphoreType.REGULAR((2,)),
            ],
            compiler_params=pltpu.CompilerParams(
                collective_id=0, has_side_effects=True, vmem_limit_bytes=60 * 1024 * 1024
            ),
        )(
            state.reshape(6, 1, count), history.reshape(3, 6, 1, count), masses.reshape(1, count)
        )
        return result.reshape(1, 6, count)

    placed = (P("level", None, "body"), P("level", None, None, "body"), P("body"))
    return jax.shard_map(
        on_device, mesh=mesh, in_specs=placed, out_specs=P("level", None, "body"), check_vma=False
    )
```
